16 devices in a mesh: fsdp: 16 (over z, y, x, core).
Axes of the slice: x: 2, y: 2, z: 2, core: 2. Of those that a mesh axis runs over, the one named last changes fastest.
Arguments:
- left_mat: bfloat16 [98304, 1536], P('fsdp')
- right_mat: bfloat16 [1536, 1536], P('fsdp')
Outputs:
- output: bfloat16 [98304, 1536], P('fsdp')
All inputs are finite; a program needn't handle non-finite values.
Results may differ from the reference program's by a relative error of at most 0.001.
Values are sent between devices in bfloat16 or wider.
A program may use at most 1 GiB of HBM per device.

```python
import jax
import jax.numpy as jnp

ROWS_TOTAL = 98304
IN_WIDTH = 1536
OUT_WIDTH = 1536


def setup_inputs(seed: int = 0) -> dict:
    base_key = jax.random.key(seed)
    key_left, key_right = jax.random.split(base_key)
    left_vals = jax.random.normal(key_left, (ROWS_TOTAL, IN_WIDTH), jnp.float32)
    right_vals = jax.random.normal(key_right, (IN_WIDTH, OUT_WIDTH), jnp.float32) * (IN_WIDTH ** -0.5)
    return {"left_mat": left_vals.astype(jnp.bfloat16), "right_mat": right_vals.astype(jnp.bfloat16)}


def reference(left_mat, right_mat):
    return jnp.dot(left_mat, right_mat, preferred_element_type=jnp.float32).astype(jnp.bfloat16)
```

```python
import jax
import jax.numpy as jnp
from jax import lax
from jax.experimental import pallas as pl
from jax.experimental.pallas import tpu as pltpu
from jax.sharding import PartitionSpec as P

MESH = pl.DeviceIdType.MESH
BF16, F32 = jnp.bfloat16, jnp.float32

W = 256
KT = 256
TM = 1024
HALF = TM // 2
SLOTS = 4
LIMIT = 20 * 2**20
FIRST = 5
PEERS = (2, 4, 8, 6, 10, 12, 14)


class Steps:
    def __init__(self, accs, a, b, flush):
        self.accs = ((accs[0], accs[1]), (accs[2], accs[3]))
        self.a, self.b, self.flush = a, b, flush
        self.n, self.last, self.staged = 0, None, False

    def push(self, unit, block, k, reg):
        pltpu.matmul_push_rhs(self.b[block, pl.ds(k * KT, KT), :], staging_register=reg, mxu_index=unit)

    def step(self, block, tile, passes, following=None):
        side = self.n % 2
        if not self.staged:
            for unit in range(2):
                self.push(unit, block, passes[0], 0)
        for p, k in enumerate(passes):
            nxt = (block, passes[p + 1]) if p + 1 < len(passes) else following
            if nxt is not None:
                reg = (p + 1) % 2 if p + 1 < len(passes) else 0
                for unit in range(2):
                    self.push(unit, *nxt, reg)
            for unit in range(2):
                rows = pl.ds(tile * TM + unit * HALF, HALF)
                pltpu.matmul_acc_lhs(
                    self.accs[unit][side], self.a[rows, pl.ds(k * KT, KT)], load_staged_rhs=p % 2
                )
        self.staged = following is not None
        self.drain()
        self.last = (block, tile, side)
        self.n += 1

    def drain(self):
        if self.last is not None:
            block, tile, side = self.last
            self.flush(block, tile, [self.accs[unit][side] for unit in range(2)])
            self.last = None


def first_kernel(blocks, a_hbm, b_hbm, a, b, c, own, load_sem, a_sem, send_sem, recv_sem, pair_sem):
    tiles, groups = a.shape[0] // TM, 4
    depth = own.shape[0]
    span = a.shape[1] // groups
    me = lax.axis_index("fsdp")
    lane, plane = lax.rem(me, 4), me // 4

    load = pltpu.make_async_copy(b_hbm, own, load_sem)
    load.start()
    barrier = pltpu.get_barrier_semaphore()
    for mask in (1, *PEERS):
        pl.semaphore_signal(barrier, inc=1, device_id=(me ^ mask,), device_id_type=MESH)

    def a_copy(tile, group):
        rows = pl.ds(tile * TM, TM)
        there = pl.ds(pl.multiple_of((plane ^ group) * span, 128), span)
        return pltpu.make_async_copy(
            a_hbm.at[rows, there], a.at[rows, pl.ds(group * span, span)], a_sem.at[tile, group]
        )

    for group in range(groups):
        for tile in range(tiles):
            a_copy(tile, group).start()

    pl.semaphore_wait(barrier, 1 + len(PEERS))
    load.wait()

    def rows_of(mask, at):
        return pl.ds(pl.multiple_of((mask // 4) * span + (lax.rem(at, 4) ^ (mask % 4)) * depth, 32), depth)

    def columns(block):
        return pl.ds(pl.multiple_of(block * W, W), W)

    def send(block, mask):
        pltpu.make_async_remote_copy(
            src_ref=own.at[:, columns(block)],
            dst_ref=b.at[block, rows_of(mask, me ^ mask), :],
            send_sem=send_sem.at[block],
            recv_sem=(pair_sem if mask == 1 else recv_sem).at[block],
            device_id=(me ^ mask,),
            device_id_type=MESH,
        ).start()

    def hand_on(block, mask):
        pltpu.make_async_remote_copy(
            src_ref=b.at[block, rows_of(mask, me), :],
            dst_ref=b.at[block, rows_of(mask, me), :],
            send_sem=send_sem.at[block],
            recv_sem=pair_sem.at[block],
            device_id=(me ^ 1,),
            device_id_type=MESH,
        ).start()

    def wait_rows(sem, block, count):
        part = b.at[block, pl.ds(0, count * depth), :]
        pltpu.make_async_copy(part, part, sem.at[block]).wait()

    def send_block(block, carry):
        for mask in (*PEERS, 1):
            send(block, mask)
        b[block, rows_of(0, me), :] = own[:, columns(block)]
        return carry

    lax.fori_loop(0, blocks, send_block, 0)

    def arrived(block):
        wait_rows(recv_sem, block, len(PEERS))
        for mask in PEERS:
            hand_on(block, mask)

    def complete(block):
        wait_rows(pair_sem, block, 1 + len(PEERS))

    def multiply(block, part):
        quarter = a.shape[0] // 4
        for piece in (2 * part, 2 * part + 1):
            rows = pl.ds(piece * quarter, quarter)
            c[block, rows, :] = jnp.dot(a[rows, :], b[block], preferred_element_type=F32).astype(BF16)

    arrived(0)
    for tile in range(tiles):
        for group in range(groups):
            a_copy(tile, group).wait()

    def one_block(block, carry):
        complete(block)
        multiply(block, 0)
        arrived(block + 1)
        multiply(block, 1)
        return carry

    lax.fori_loop(0, FIRST, one_block, 0)
    for block in range(FIRST, blocks):
        if block > FIRST:
            arrived(block)
        complete(block)
    for block in range(blocks):
        wait_rows(send_sem, block, 1 + 2 * len(PEERS))


def second_kernel(blocks, a, b, c, out, stage, out_sem, c_sem):
    tiles = a.shape[0] // TM

    def done_copy(block):
        return pltpu.make_async_copy(c.at[block], out.at[:, pl.ds(block * W, W)], c_sem.at[block])

    for block in range(FIRST):
        done_copy(block).start()

    used = []

    def out_copy(block, tile, slot):
        return pltpu.make_async_copy(
            stage.at[slot], out.at[pl.ds(tile * TM, TM), pl.ds(block * W, W)], out_sem.at[slot]
        )

    def flush(block, tile, accs):
        n = len(used)
        slot = n % SLOTS
        for unit in range(2):
            stage[slot, pl.ds(unit * HALF, HALF), :] = pltpu.matmul_pop(accs[unit]).astype(BF16)
        out_copy(block, tile, slot).start()
        used.append((block, tile, slot))

    def body(*accs):
        steps = Steps(accs, a, b, flush)
        order = [(block, tile) for block in range(FIRST, blocks) for tile in range(tiles)]
        for at, (block, tile) in enumerate(order):
            if at > SLOTS:
                out_copy(*used[at - 1 - SLOTS]).wait()
            steps.step(block, tile, range(6), (order[at + 1][0], 0) if at + 1 < len(order) else None)
        if len(order) > SLOTS:
            out_copy(*used[len(order) - 1 - SLOTS]).wait()
        steps.drain()
        for copy in used[max(0, len(order) - SLOTS) :]:
            out_copy(*copy).wait()

    pl.run_scoped(body, *[pltpu.ACC(unit)((HALF, W), F32) for unit in (0, 0, 1, 1)])
    for block in range(FIRST):
        done_copy(block).wait()


def solution(mesh):
    def step(a, b):
        (rows, depth), (own, columns) = a.shape, b.shape
        blocks, tiles = columns // W, rows // TM
        dma = pltpu.SemaphoreType.DMA
        vmem, hbm = pl.BlockSpec(memory_space=pltpu.VMEM), pl.BlockSpec(memory_space=pltpu.HBM)
        a, b, c = pl.pallas_call(
            lambda *refs: first_kernel(blocks, *refs),
            name="first",
            out_shape=(
                pltpu.VMEM((rows, depth), BF16),
                pltpu.VMEM((blocks, depth, W), BF16),
                pltpu.VMEM((FIRST, rows, W), BF16),
            ),
            in_specs=[hbm, hbm],
            out_specs=(vmem, vmem, vmem),
            scratch_shapes=[
                pltpu.VMEM((own, columns), BF16),
                dma,
                dma((tiles, 4)),
                dma((blocks,)),
                dma((blocks,)),
                dma((blocks,)),
            ],
            compiler_params=pltpu.CompilerParams(
                vmem_limit_bytes=LIMIT, collective_id=0, has_side_effects=True
            ),
        )(a, b)
        a, b, c = (pltpu.with_memory_space_constraint(x, pltpu.VMEM) for x in (a, b, c))
        return pl.pallas_call(
            lambda *refs: second_kernel(blocks, *refs),
            name="second",
            out_shape=jax.ShapeDtypeStruct((rows, columns), BF16),
            in_specs=[vmem, vmem, vmem],
            out_specs=hbm,
            scratch_shapes=[pltpu.VMEM((SLOTS, TM, W), BF16), dma((SLOTS,)), dma((FIRST,))],
            compiler_params=pltpu.CompilerParams(vmem_limit_bytes=LIMIT),
        )(a, b, c)

    spec = P("fsdp", None)
    return jax.shard_map(step, mesh=mesh, in_specs=(spec, spec), out_specs=spec, check_vma=False)
```

```python
import functools

import jax
import jax.numpy as jnp
from jax import lax
from jax.experimental import pallas as pl
from jax.experimental.pallas import tpu as pltpu
from jax.sharding import PartitionSpec as P

MESH = pl.DeviceIdType.MESH
BF16, F32 = jnp.bfloat16, jnp.float32

W = 256
KT = 256
TM = 1024
HALF = TM // 2
SLOTS = 8
LIMIT = 20 * 2**20
WHOLE = 4
PART = 4
NEAR, FAR = (2, 4, 6), (8, 10, 12, 14)
PEERS = NEAR + FAR


class Steps:
    def __init__(self, accs, a, b, flush):
        self.accs = ((accs[0], accs[1]), (accs[2], accs[3]))
        self.a, self.b, self.flush = a, b, flush
        self.n, self.last, self.staged = 0, None, False

    def push(self, unit, block, k, reg):
        pltpu.matmul_push_rhs(self.b[block, pl.ds(k * KT, KT), :], staging_register=reg, mxu_index=unit)

    def step(self, block, tile, passes, following=None):
        side = self.n % 2
        if not self.staged:
            for unit in range(2):
                self.push(unit, block, passes[0], 0)
        for p, k in enumerate(passes):
            nxt = (block, passes[p + 1]) if p + 1 < len(passes) else following
            if nxt is not None:
                reg = (p + 1) % 2 if p + 1 < len(passes) else 0
                for unit in range(2):
                    self.push(unit, *nxt, reg)
            for unit in range(2):
                rows = pl.ds(tile * TM + unit * HALF, HALF)
                pltpu.matmul_acc_lhs(
                    self.accs[unit][side], self.a[rows, pl.ds(k * KT, KT)], load_staged_rhs=p % 2
                )
        self.staged = following is not None
        self.drain()
        self.last = (block, tile, side)
        self.n += 1

    def drain(self):
        if self.last is not None:
            block, tile, side = self.last
            self.flush(block, tile, [self.accs[unit][side] for unit in range(2)])
            self.last = None


def first_kernel(blocks, a_hbm, b_hbm, a, b, c, own, partial, load_sem, a_sem, send_sem, recv_sem, pair_sem):
    tiles, groups = a.shape[0] // TM, 4
    depth = own.shape[0]
    span = a.shape[1] // groups
    me = lax.axis_index("fsdp")
    plane = me // 4

    load = pltpu.make_async_copy(b_hbm, own, load_sem)
    load.start()
    barrier = pltpu.get_barrier_semaphore()
    for mask in (1, *PEERS):
        pl.semaphore_signal(barrier, inc=1, device_id=(me ^ mask,), device_id_type=MESH)

    def a_copy(tile, group):
        rows = pl.ds(tile * TM, TM)
        there = pl.ds(pl.multiple_of((plane ^ group) * span, 128), span)
        return pltpu.make_async_copy(
            a_hbm.at[rows, there], a.at[rows, pl.ds(group * span, span)], a_sem.at[tile, group]
        )

    for group in range(groups):
        for tile in range(tiles):
            a_copy(tile, group).start()

    pl.semaphore_wait(barrier, 1 + len(PEERS))
    load.wait()

    def rows_of(mask, at):
        return pl.ds(pl.multiple_of((mask // 4) * span + (at % 4 ^ mask % 4) * depth, 32), depth)

    def columns(block):
        return pl.ds(pl.multiple_of(block * W, W), W)

    first = me % 8 - me % 2

    def send(block, mask, half):
        pltpu.make_async_remote_copy(
            src_ref=own.at[:, columns(block)],
            dst_ref=b.at[block, rows_of(mask, me ^ mask), :],
            send_sem=send_sem.at[block],
            recv_sem=(pair_sem if isinstance(mask, int) else recv_sem).at[block, half],
            device_id=(me ^ mask,),
            device_id_type=MESH,
        ).start()

    def wait_rows(sem, block, count):
        part = b.at[block, pl.ds(0, count * depth), :]
        pltpu.make_async_copy(part, part, sem).wait()

    def send_block(block, carry):
        for turn in (0, 2, 4, 6):
            mask = first ^ turn
            pl.when(mask != 0)(functools.partial(send, block, mask, 0))
        send(block, 1, 0)
        for turn in (0, 2, 4, 6):
            send(block, 8 + (first ^ turn), 1)
        b[block, rows_of(0, me), :] = own[:, columns(block)]
        return carry

    lax.fori_loop(0, blocks, send_block, 0)

    def arrived(block, half):
        masks = (NEAR, FAR)[half]
        wait_rows(recv_sem.at[block, half], block, len(masks))
        for mask in masks:
            pltpu.make_async_remote_copy(
                src_ref=b.at[block, rows_of(mask, me), :],
                dst_ref=b.at[block, rows_of(mask, me), :],
                send_sem=send_sem.at[block],
                recv_sem=pair_sem.at[block, half],
                device_id=(me ^ 1,),
                device_id_type=MESH,
            ).start()

    def complete(block, half):
        wait_rows(pair_sem.at[block, half], block, 4)

    middle = 2 * span

    def dots(first, count, each):
        for piece in range(2):
            each(pl.ds(first + piece * (count // 2), count // 2))

    def near(block, first, count):
        def each(rows):
            partial[rows, :] = jnp.dot(a[rows, :middle], b[block, :middle, :], preferred_element_type=F32)

        dots(first, count, each)

    def far(block, first, count):
        def each(rows):
            product = jnp.dot(a[rows, middle:], b[block, middle:, :], preferred_element_type=F32)
            c[block, rows, :] = (partial[rows, :] + product).astype(BF16)

        dots(first, count, each)

    total = a.shape[0]
    part = total // 2

    arrived(0, 0)
    for tile in range(tiles):
        for group in range(groups):
            a_copy(tile, group).wait()

    complete(0, 0)
    near(0, 0, part)
    arrived(0, 1)
    near(0, part, part)
    complete(0, 1)
    far(0, 0, part)
    arrived(1, 0)
    far(0, part, part)

    def one_block(block, carry):
        complete(block, 0)
        arrived(block, 1)
        near(block, 0, total)
        complete(block, 1)
        arrived(block + 1, 0)
        far(block, 0, total)
        return carry

    lax.fori_loop(1, WHOLE, one_block, 0)
    rows = PART * TM
    complete(WHOLE, 0)
    arrived(WHOLE, 1)
    near(WHOLE, 0, rows)
    complete(WHOLE, 1)
    arrived(WHOLE + 1, 0)
    far(WHOLE, 0, rows // 2)
    arrived(WHOLE + 1, 1)
    far(WHOLE, rows // 2, rows // 2)
    complete(WHOLE + 1, 0)
    complete(WHOLE + 1, 1)
    for block in range(blocks):
        wait_rows(send_sem.at[block], block, 1 + 2 * len(PEERS))


def second_kernel(blocks, a, b, c, out, stage, out_sem, c_sem):
    tiles = a.shape[0] // TM

    def done_copy(block):
        rows = pl.ds(0, a.shape[0] if block < WHOLE else PART * TM)
        return pltpu.make_async_copy(
            c.at[block, rows, :], out.at[rows, pl.ds(block * W, W)], c_sem.at[block]
        )

    for block in range(WHOLE + 1):
        done_copy(block).start()

    used = []

    def out_copy(block, tile, slot):
        return pltpu.make_async_copy(
            stage.at[slot], out.at[pl.ds(tile * TM, TM), pl.ds(block * W, W)], out_sem.at[slot]
        )

    def flush(block, tile, accs):
        n = len(used)
        slot = n % SLOTS
        for unit in range(2):
            stage[slot, pl.ds(unit * HALF, HALF), :] = pltpu.matmul_pop(accs[unit]).astype(BF16)
        out_copy(block, tile, slot).start()
        used.append((block, tile, slot))

    def body(*accs):
        steps = Steps(accs, a, b, flush)
        order = [(WHOLE, tile) for tile in range(PART, tiles)]
        order += [(block, tile) for block in range(WHOLE + 1, blocks) for tile in range(tiles)]
        for at, (block, tile) in enumerate(order):
            if at > SLOTS:
                out_copy(*used[at - 1 - SLOTS]).wait()
            steps.step(block, tile, range(6), (order[at + 1][0], 0) if at + 1 < len(order) else None)
        if len(order) > SLOTS:
            out_copy(*used[len(order) - 1 - SLOTS]).wait()
        steps.drain()
        for copy in used[max(0, len(order) - SLOTS) :]:
            out_copy(*copy).wait()

    pl.run_scoped(body, *[pltpu.ACC(unit)((HALF, W), F32) for unit in (0, 0, 1, 1)])
    for block in range(WHOLE + 1):
        done_copy(block).wait()


def solution(mesh):
    def step(a, b):
        (rows, depth), (own, columns) = a.shape, b.shape
        blocks, tiles = columns // W, rows // TM
        dma = pltpu.SemaphoreType.DMA
        vmem, hbm = pl.BlockSpec(memory_space=pltpu.VMEM), pl.BlockSpec(memory_space=pltpu.HBM)
        a, b, c = pl.pallas_call(
            lambda *refs: first_kernel(blocks, *refs),
            name="first",
            out_shape=(
                pltpu.VMEM((rows, depth), BF16),
                pltpu.VMEM((blocks, depth, W), BF16),
                pltpu.VMEM((WHOLE + 1, rows, W), BF16),
            ),
            in_specs=[hbm, hbm],
            out_specs=(vmem, vmem, vmem),
            scratch_shapes=[
                pltpu.VMEM((own, columns), BF16),
                pltpu.VMEM((rows, W), F32),
                dma,
                dma((tiles, 4)),
                dma((blocks,)),
                dma((blocks, 2)),
                dma((blocks, 2)),
            ],
            compiler_params=pltpu.CompilerParams(
                vmem_limit_bytes=LIMIT, collective_id=0, has_side_effects=True
            ),
        )(a, b)
        a, b, c = (pltpu.with_memory_space_constraint(x, pltpu.VMEM) for x in (a, b, c))
        return pl.pallas_call(
            lambda *refs: second_kernel(blocks, *refs),
            name="second",
            out_shape=jax.ShapeDtypeStruct((rows, columns), BF16),
            in_specs=[vmem, vmem, vmem],
            out_specs=hbm,
            scratch_shapes=[pltpu.VMEM((SLOTS, TM, W), BF16), dma((SLOTS,)), dma((WHOLE + 1,))],
            compiler_params=pltpu.CompilerParams(vmem_limit_bytes=LIMIT),
        )(a, b, c)

    spec = P("fsdp", None)
    return jax.shard_map(step, mesh=mesh, in_specs=(spec, spec), out_specs=spec, check_vma=False)
```

```python
import functools

import jax
import jax.numpy as jnp
from jax import lax
from jax.experimental import pallas as pl
from jax.experimental.pallas import tpu as pltpu
from jax.sharding import PartitionSpec as P

MESH = pl.DeviceIdType.MESH
BF16, F32 = jnp.bfloat16, jnp.float32

W = 256
KT = 256
TM = 1024
STEP = 512
HALF = STEP // 2
LIMIT = 20 * 2**20
WHOLE = 4
EARLY = 4
PART = 4
NEAR, FAR = (2, 4, 6), (14, 10, 12, 8)
PEERS = NEAR + FAR
PAIR = 1
GREETED = (1, 2, 4, 6, 8)


class Steps:
    def __init__(self, accs, a, b, flush):
        self.accs = ((accs[0], accs[1]), (accs[2], accs[3]))
        self.a, self.b, self.flush = a, b, flush
        self.n, self.last, self.staged = 0, None, False

    def push(self, unit, block, k, reg):
        pltpu.matmul_push_rhs(self.b[block, pl.ds(k * KT, KT), :], staging_register=reg, mxu_index=unit)

    def step(self, block, tile, passes, following=None):
        side = self.n % 2
        if not self.staged:
            for unit in range(2):
                self.push(unit, block, passes[0], 0)
        for p, k in enumerate(passes):
            nxt = (block, passes[p + 1]) if p + 1 < len(passes) else following
            if nxt is not None:
                reg = (p + 1) % 2 if p + 1 < len(passes) else 0
                for unit in range(2):
                    self.push(unit, *nxt, reg)
            for unit in range(2):
                rows = pl.ds(tile * STEP + unit * HALF, HALF)
                pltpu.matmul_acc_lhs(
                    self.accs[unit][side], self.a[rows, pl.ds(k * KT, KT)], load_staged_rhs=p % 2
                )
        self.staged = following is not None
        self.drain()
        self.last = (block, tile, side)
        self.n += 1

    def drain(self):
        if self.last is not None:
            block, tile, side = self.last
            self.flush(block, tile, [self.accs[unit][side] for unit in range(2)])
            self.last = None


def first_kernel(blocks, a_hbm, b_hbm, a, b, c, partial, load_sem, a_sem, send_sem, recv_sem, pair_sem, ready):
    tiles, groups = a.shape[0] // TM, 4
    depth = b_hbm.shape[0]
    span = a.shape[1] // groups
    me = lax.axis_index("fsdp")
    plane = me // 4

    def rows_of(mask, at):
        return pl.ds(pl.multiple_of((mask // 4) * span + (at % 4 ^ mask % 4) * depth, 32), depth)

    def load(block):
        there = pl.ds(pl.multiple_of(block * W, W), W)
        return pltpu.make_async_copy(b_hbm.at[:, there], b.at[block, rows_of(0, me), :], load_sem.at[block])

    for block in range(blocks):
        load(block).start()
    barrier = pltpu.get_barrier_semaphore()
    for mask in GREETED:
        pl.semaphore_signal(barrier, inc=1, device_id=(me ^ mask,), device_id_type=MESH)

    def a_copy(tile, group):
        rows = pl.ds(tile * TM, TM)
        there = pl.ds(pl.multiple_of((plane ^ group) * span, 128), span)
        return pltpu.make_async_copy(
            a_hbm.at[rows, there], a.at[rows, pl.ds(group * span, span)], a_sem.at[tile, group]
        )

    for group in range(groups):
        for tile in range(tiles):
            a_copy(tile, group).start()

    pl.semaphore_wait(barrier, len(GREETED))
    pl.semaphore_signal(ready, inc=1, device_id=(me ^ 8,), device_id_type=MESH)
    load(0).wait()

    first = me % 8 - me % 2

    def send(block, mask, half):
        pltpu.make_async_remote_copy(
            src_ref=b.at[block, rows_of(0, me), :],
            dst_ref=b.at[block, rows_of(mask, me ^ mask), :],
            send_sem=send_sem.at[block],
            recv_sem=recv_sem.at[block, half],
            device_id=(me ^ mask,),
            device_id_type=MESH,
        ).start()

    chips = b.reshape(blocks, 8, 2 * depth, W)

    def wait_rows(sem, block, count):
        part = b.at[block, pl.ds(0, count * depth), :]
        pltpu.make_async_copy(part, part, sem).wait()

    def send_near(block):
        for turn in (0, 2, 4, 6):
            mask = first ^ turn
            pl.when(mask != 0)(functools.partial(send, block, mask, 0))

    def send_far(block):
        for mask in (14, 10, 12, 8):
            send(block, mask, 1)

    def send_block(block, carry):
        load(block).wait()
        send_near(block)
        send_far(block)
        return carry

    send_near(0)
    pl.semaphore_wait(ready, 1)
    send_far(0)
    lax.fori_loop(1, blocks, send_block, 0)

    def arrived(block, half):
        wait_rows(recv_sem.at[block, half], block, len((NEAR, FAR)[half]))
        mine = chips.at[block, pl.ds(4 * half, 4), pl.ds(pl.multiple_of(me % 2 * depth, 32), depth), :]
        pltpu.make_async_remote_copy(
            src_ref=mine,
            dst_ref=mine,
            send_sem=send_sem.at[block],
            recv_sem=pair_sem.at[block, half],
            device_id=(me ^ PAIR,),
            device_id_type=MESH,
        ).start()

    def complete(block, half):
        wait_rows(pair_sem.at[block, half], block, 4)

    middle = 2 * span

    def dots(first, count, each):
        for piece in range(2):
            each(pl.ds(first + piece * (count // 2), count // 2))

    def near(block, first, count):
        def each(rows):
            partial[rows, :] = jnp.dot(a[rows, :middle], b[block, :middle, :], preferred_element_type=F32)

        dots(first, count, each)

    def full(block, first, count):
        def each(rows):
            c[block, rows, :] = jnp.dot(a[rows, :], b[block], preferred_element_type=F32).astype(BF16)

        dots(first, count, each)

    def far(block, first, count):
        def each(rows):
            product = jnp.dot(a[rows, middle:], b[block, middle:, :], preferred_element_type=F32)
            c[block, rows, :] = (partial[rows, :] + product).astype(BF16)

        dots(first, count, each)

    total = a.shape[0]
    part = total // 2

    arrived(0, 0)
    for tile in range(tiles):
        for group in range(groups):
            a_copy(tile, group).wait()

    early = EARLY * TM
    complete(0, 0)
    near(0, 0, early)
    arrived(0, 1)
    near(0, early, total - early)
    complete(0, 1)
    far(0, 0, part)
    arrived(1, 0)
    far(0, part, part)

    def one_block(block, carry):
        complete(block, 0)
        arrived(block, 1)
        near(block, 0, total)
        complete(block, 1)
        arrived(block + 1, 0)
        pl.when(block + 1 == WHOLE)(lambda: arrived(WHOLE, 1))
        far(block, 0, total)
        return carry

    lax.fori_loop(1, WHOLE, one_block, 0)
    rows = PART * TM // 2
    complete(WHOLE, 0)
    complete(WHOLE, 1)
    full(WHOLE, 0, rows)
    arrived(WHOLE + 1, 0)
    arrived(WHOLE + 1, 1)
    full(WHOLE, rows, rows)
    complete(WHOLE + 1, 0)
    complete(WHOLE + 1, 1)
    for block in range(blocks):
        wait_rows(send_sem.at[block], block, 1 + 2 * len(PEERS))


def second_steps(blocks, rows):
    left = [(WHOLE, step) for step in range(PART * TM // STEP, rows // STEP)]
    return left + [(block, step) for block in range(WHOLE + 1, blocks) for step in range(rows // STEP)]


def second_kernel(blocks, a, b, c, out, stage, out_sem, c_sem):
    order = second_steps(blocks, a.shape[0])

    def done_copy(block):
        rows = pl.ds(0, a.shape[0] if block < WHOLE else PART * TM)
        return pltpu.make_async_copy(
            c.at[block, rows, :], out.at[rows, pl.ds(block * W, W)], c_sem.at[block]
        )

    for block in range(WHOLE + 1):
        done_copy(block).start()

    def out_copy(slot):
        block, step = order[slot]
        return pltpu.make_async_copy(
            stage.at[slot], out.at[pl.ds(step * STEP, STEP), pl.ds(block * W, W)], out_sem.at[slot]
        )

    def flush(block, step, accs):
        slot = order.index((block, step))
        for unit in range(2):
            stage[slot, pl.ds(unit * HALF, HALF), :] = pltpu.matmul_pop(accs[unit]).astype(BF16)
        out_copy(slot).start()

    def body(*accs):
        steps = Steps(accs, a, b, flush)
        for at, (block, step) in enumerate(order):
            steps.step(block, step, range(6), (order[at + 1][0], 0) if at + 1 < len(order) else None)
        steps.drain()

    pl.run_scoped(body, *[pltpu.ACC(unit)((HALF, W), F32) for unit in (0, 0, 1, 1)])
    for slot in range(len(order)):
        out_copy(slot).wait()
    for block in range(WHOLE + 1):
        done_copy(block).wait()


def solution(mesh):
    def step(a, b):
        (rows, depth), columns = a.shape, b.shape[1]
        blocks, tiles = columns // W, rows // TM
        slots = len(second_steps(blocks, rows))
        dma = pltpu.SemaphoreType.DMA
        vmem, hbm = pl.BlockSpec(memory_space=pltpu.VMEM), pl.BlockSpec(memory_space=pltpu.HBM)
        a, b, c = pl.pallas_call(
            lambda *refs: first_kernel(blocks, *refs),
            name="first",
            out_shape=(
                pltpu.VMEM((rows, depth), BF16),
                pltpu.VMEM((blocks, depth, W), BF16),
                pltpu.VMEM((WHOLE + 1, rows, W), BF16),
            ),
            in_specs=[hbm, hbm],
            out_specs=(vmem, vmem, vmem),
            scratch_shapes=[
                pltpu.VMEM((rows, W), F32),
                dma((blocks,)),
                dma((tiles, 4)),
                dma((blocks,)),
                dma((blocks, 2)),
                dma((blocks, 2)),
                pltpu.SemaphoreType.REGULAR,
            ],
            compiler_params=pltpu.CompilerParams(
                vmem_limit_bytes=LIMIT, collective_id=0, has_side_effects=True
            ),
        )(a, b)
        a, b, c = (pltpu.with_memory_space_constraint(x, pltpu.VMEM) for x in (a, b, c))
        return pl.pallas_call(
            lambda *refs: second_kernel(blocks, *refs),
            name="second",
            out_shape=jax.ShapeDtypeStruct((rows, columns), BF16),
            in_specs=[vmem, vmem, vmem],
            out_specs=hbm,
            scratch_shapes=[pltpu.VMEM((slots, STEP, W), BF16), dma((slots,)), dma((WHOLE + 1,))],
            compiler_params=pltpu.CompilerParams(vmem_limit_bytes=LIMIT),
        )(a, b, c)

    spec = P("fsdp", None)
    return jax.shard_map(step, mesh=mesh, in_specs=(spec, spec), out_specs=spec, check_vma=False)
```

```python
import functools

import jax
import jax.numpy as jnp
from jax import lax
from jax.experimental import pallas as pl
from jax.experimental.pallas import tpu as pltpu
from jax.sharding import PartitionSpec as P

MESH = pl.DeviceIdType.MESH
BF16, F32 = jnp.bfloat16, jnp.float32

W = 256
KT = 256
TM = 1024
STEP = 512
HALF = STEP // 2
LIMIT = 20 * 2**20
WHOLE = 4
EARLY = 4
PART = 4
NEAR, FAR = (2, 4, 6), (14, 10, 12, 8)
PEERS = NEAR + FAR
PAIR = 1
GREETED = (1, 2, 4, 6, 8)


class Steps:
    def __init__(self, accs, a, b, flush):
        self.accs = ((accs[0], accs[1]), (accs[2], accs[3]))
        self.a, self.b, self.flush = a, b, flush
        self.n, self.last, self.staged = 0, None, False

    def push(self, unit, block, k, reg):
        pltpu.matmul_push_rhs(self.b[block, pl.ds(k * KT, KT), :], staging_register=reg, mxu_index=unit)

    def step(self, block, tile, passes, following=None):
        side = self.n % 2
        if not self.staged:
            for unit in range(2):
                self.push(unit, block, passes[0], 0)
        for p, k in enumerate(passes):
            nxt = (block, passes[p + 1]) if p + 1 < len(passes) else following
            if nxt is not None:
                reg = (p + 1) % 2 if p + 1 < len(passes) else 0
                for unit in range(2):
                    self.push(unit, *nxt, reg)
            for unit in range(2):
                rows = pl.ds(tile * STEP + unit * HALF, HALF)
                pltpu.matmul_acc_lhs(
                    self.accs[unit][side], self.a[rows, pl.ds(k * KT, KT)], load_staged_rhs=p % 2
                )
        self.staged = following is not None
        self.drain()
        self.last = (block, tile, side)
        self.n += 1

    def drain(self):
        if self.last is not None:
            block, tile, side = self.last
            self.flush(block, tile, [self.accs[unit][side] for unit in range(2)])
            self.last = None


def first_kernel(blocks, a_hbm, b_hbm, a, b, c, partial, load_sem, a_sem, send_sem, recv_sem, pair_sem, ready):
    tiles, groups = a.shape[0] // TM, 4
    depth = b_hbm.shape[0]
    span = a.shape[1] // groups
    me = lax.axis_index("fsdp")
    plane = me // 4

    def rows_of(mask, at):
        return pl.ds(pl.multiple_of((mask // 4) * span + (at % 4 ^ mask % 4) * depth, 32), depth)

    def load(block):
        there = pl.ds(pl.multiple_of(block * W, W), W)
        return pltpu.make_async_copy(b_hbm.at[:, there], b.at[block, rows_of(0, me), :], load_sem.at[block])

    for block in range(blocks):
        load(block).start()
    barrier = pltpu.get_barrier_semaphore()
    for mask in GREETED:
        pl.semaphore_signal(barrier, inc=1, device_id=(me ^ mask,), device_id_type=MESH)

    def a_copy(tile, group):
        rows = pl.ds(tile * TM, TM)
        there = pl.ds(pl.multiple_of((plane ^ group) * span, 128), span)
        return pltpu.make_async_copy(
            a_hbm.at[rows, there], a.at[rows, pl.ds(group * span, span)], a_sem.at[tile, group]
        )

    for group in range(groups):
        for tile in range(tiles):
            a_copy(tile, group).start()

    pl.semaphore_wait(barrier, len(GREETED))
    pl.semaphore_signal(ready, inc=1, device_id=(me ^ 8,), device_id_type=MESH)
    load(0).wait()

    first = me % 8 - me % 2

    def send(block, mask, half):
        pltpu.make_async_remote_copy(
            src_ref=b.at[block, rows_of(0, me), :],
            dst_ref=b.at[block, rows_of(mask, me ^ mask), :],
            send_sem=send_sem.at[block],
            recv_sem=recv_sem.at[block, half],
            device_id=(me ^ mask,),
            device_id_type=MESH,
        ).start()

    chips = b.reshape(blocks, 8, 2 * depth, W)

    def wait_rows(sem, block, count):
        part = b.at[block, pl.ds(0, count * depth), :]
        pltpu.make_async_copy(part, part, sem).wait()

    def send_near(block):
        for turn in (0, 2, 4, 6):
            mask = first ^ turn
            pl.when(mask != 0)(functools.partial(send, block, mask, 0))

    def send_far(block):
        for mask in (14, 10, 12, 8):
            send(block, mask, 1)

    def send_block(block, carry):
        load(block).wait()
        send_near(block)
        send_far(block)
        return carry

    send_near(0)
    pl.semaphore_wait(ready, 1)
    send_far(0)
    lax.fori_loop(1, blocks, send_block, 0)

    def arrived(block, half):
        wait_rows(recv_sem.at[block, half], block, len((NEAR, FAR)[half]))
        mine = chips.at[block, pl.ds(4 * half, 4), pl.ds(pl.multiple_of(me % 2 * depth, 32), depth), :]
        pltpu.make_async_remote_copy(
            src_ref=mine,
            dst_ref=mine,
            send_sem=send_sem.at[block],
            recv_sem=pair_sem.at[block, half],
            device_id=(me ^ PAIR,),
            device_id_type=MESH,
        ).start()

    def complete(block, half):
        wait_rows(pair_sem.at[block, half], block, 4)

    middle = 2 * span

    def dots(first, count, each):
        for piece in range(2):
            each(pl.ds(first + piece * (count // 2), count // 2))

    def near(block, first, count):
        def each(rows):
            partial[rows, :] = jnp.dot(a[rows, :middle], b[block, :middle, :], preferred_element_type=F32)

        dots(first, count, each)

    def full(block, first, count):
        def each(rows):
            c[block, rows, :] = jnp.dot(a[rows, :], b[block], preferred_element_type=F32).astype(BF16)

        dots(first, count, each)

    def far(block, first, count):
        def each(rows):
            product = jnp.dot(a[rows, middle:], b[block, middle:, :], preferred_element_type=F32)
            c[block, rows, :] = (partial[rows, :] + product).astype(BF16)

        dots(first, count, each)

    total = a.shape[0]

    arrived(0, 0)
    for tile in range(tiles):
        for group in range(groups):
            a_copy(tile, group).wait()

    early = EARLY * TM
    complete(0, 0)
    near(0, 0, early)
    arrived(0, 1)
    near(0, early, total - early)
    complete(0, 1)
    arrived(1, 0)
    far(0, 0, total)

    def one_block(block, carry):
        complete(block, 0)
        arrived(block, 1)
        near(block, 0, total)
        complete(block, 1)
        arrived(block + 1, 0)
        pl.when(block + 1 == WHOLE)(lambda: arrived(WHOLE, 1))
        far(block, 0, total)
        return carry

    lax.fori_loop(1, WHOLE, one_block, 0)
    rows = PART * TM // 2
    complete(WHOLE, 0)
    complete(WHOLE, 1)
    full(WHOLE, 0, rows)
    arrived(WHOLE + 1, 0)
    arrived(WHOLE + 1, 1)
    full(WHOLE, rows, rows)
    complete(WHOLE + 1, 0)
    complete(WHOLE + 1, 1)
    for block in range(blocks):
        wait_rows(send_sem.at[block], block, 1 + 2 * len(PEERS))


def second_steps(blocks, rows):
    left = [(WHOLE, step) for step in range(PART * TM // STEP, rows // STEP)]
    return left + [(block, step) for block in range(WHOLE + 1, blocks) for step in range(rows // STEP)]


def second_kernel(blocks, a, b, c, out, stage, out_sem, c_sem):
    order = second_steps(blocks, a.shape[0])

    def done_copy(block):
        rows = pl.ds(0, a.shape[0] if block < WHOLE else PART * TM)
        return pltpu.make_async_copy(
            c.at[block, rows, :], out.at[rows, pl.ds(block * W, W)], c_sem.at[block]
        )

    for block in range(WHOLE + 1):
        done_copy(block).start()

    def out_copy(slot):
        block, step = order[slot]
        return pltpu.make_async_copy(
            stage.at[slot], out.at[pl.ds(step * STEP, STEP), pl.ds(block * W, W)], out_sem.at[slot]
        )

    def flush(block, step, accs):
        slot = order.index((block, step))
        for unit in range(2):
            stage[slot, pl.ds(unit * HALF, HALF), :] = pltpu.matmul_pop(accs[unit]).astype(BF16)
        out_copy(slot).start()

    def body(*accs):
        steps = Steps(accs, a, b, flush)
        for at, (block, step) in enumerate(order):
            steps.step(block, step, range(6), (order[at + 1][0], 0) if at + 1 < len(order) else None)
        steps.drain()

    pl.run_scoped(body, *[pltpu.ACC(unit)((HALF, W), F32) for unit in (0, 0, 1, 1)])
    for slot in range(len(order)):
        out_copy(slot).wait()
    for block in range(WHOLE + 1):
        done_copy(block).wait()


def solution(mesh):
    def step(a, b):
        (rows, depth), columns = a.shape, b.shape[1]
        blocks, tiles = columns // W, rows // TM
        slots = len(second_steps(blocks, rows))
        dma = pltpu.SemaphoreType.DMA
        vmem, hbm = pl.BlockSpec(memory_space=pltpu.VMEM), pl.BlockSpec(memory_space=pltpu.HBM)
        a, b, c = pl.pallas_call(
            lambda *refs: first_kernel(blocks, *refs),
            name="first",
            out_shape=(
                pltpu.VMEM((rows, depth), BF16),
                pltpu.VMEM((blocks, depth, W), BF16),
                pltpu.VMEM((WHOLE + 1, rows, W), BF16),
            ),
            in_specs=[hbm, hbm],
            out_specs=(vmem, vmem, vmem),
            scratch_shapes=[
                pltpu.VMEM((rows, W), F32),
                dma((blocks,)),
                dma((tiles, 4)),
                dma((blocks,)),
                dma((blocks, 2)),
                dma((blocks, 2)),
                pltpu.SemaphoreType.REGULAR,
            ],
            compiler_params=pltpu.CompilerParams(
                vmem_limit_bytes=LIMIT, collective_id=0, has_side_effects=True
            ),
        )(a, b)
        a, b, c = (pltpu.with_memory_space_constraint(x, pltpu.VMEM) for x in (a, b, c))
        return pl.pallas_call(
            lambda *refs: second_kernel(blocks, *refs),
            name="second",
            out_shape=jax.ShapeDtypeStruct((rows, columns), BF16),
            in_specs=[vmem, vmem, vmem],
            out_specs=hbm,
            scratch_shapes=[pltpu.VMEM((slots, STEP, W), BF16), dma((slots,)), dma((WHOLE + 1,))],
            compiler_params=pltpu.CompilerParams(vmem_limit_bytes=LIMIT),
        )(a, b, c)

    spec = P("fsdp", None)
    return jax.shard_map(step, mesh=mesh, in_specs=(spec, spec), out_specs=spec, check_vma=False)
```
